32 devices in a mesh: dp: 8 (over y, x, core), tp: 4 (over z).
Axes of the slice: x: 2, y: 2, z: 4, core: 2. Of those that a mesh axis runs over, the one named last changes fastest.
Arguments:
- inputs: bfloat16 [8, 768, 1280], P('dp', 'tp'), may hold values from -6 to 6
- saved_hidden: bfloat16 [8, 768, 5120], P('dp', None, 'tp'), may hold values from -8 to 8
- upstream: bfloat16 [8, 768, 1280], P('dp', 'tp'), may hold values from -6 to 6
- w_in: bfloat16 [1280, 5120], P(None, 'tp'), may hold values from -0.15625 to 0.15625
- w_out: bfloat16 [5120, 1280], P('tp'), may hold values from -0.078125 to 0.078125
- kernel: float32 [7, 1280], replicated, may hold values from -2 to 2
Outputs:
- grad_inputs: bfloat16 [8, 768, 1280], P('dp', 'tp')
- grad_w_in: float32 [1280, 5120], P(None, 'tp')
- grad_w_out: float32 [5120, 1280], P('tp')
- grad_bias: float32 [5120], P('tp')
- grad_kernel: float32 [7, 1280], replicated
The draws below stay inside these ranges and needn't reach their ends.
All inputs are finite; a program needn't handle non-finite values.
Results may differ from the reference program's by a relative error of at most 0.02.
Values may be sent and summed in bfloat16 or wider, within the bound.
No kernel may reach another device: no remote copies, remote signals or barrier semaphores. Data moves between devices by JAX's collectives and lax.ppermute only.
A program may use at most 128 MiB of HBM per device.

```python
from functools import partial
import jax
import jax.numpy as jnp
from jax import lax

D = 1280
FF = 5120
KW = 7
SEQ = 768
SEQS = 8
N_TP = 4


def shard_levels(stream_key, dims, pieces, low, top_value):
    gain = 1.0
    for position, blocks in pieces:
        draws = jax.random.uniform(jax.random.fold_in(jax.random.fold_in(stream_key, 6), position), (blocks,), jnp.float32, low / len(pieces), top_value / len(pieces))
        gain = gain * jnp.repeat(jnp.exp(draws), dims[position] // blocks).reshape((-1,) + (1,) * (len(dims) - 1 - position))
    return gain


def normal_values(rng, dims, width, reach, split=(), dtype=jnp.bfloat16):
    values = width * jax.random.normal(rng, dims, jnp.float32)
    if split:
        values = values * shard_levels(rng, dims, split, -0.22, 0.18)
    return jnp.clip(values, -reach, reach).astype(dtype)


def setup_inputs(seed: int = 0) -> dict:
    key_of = jax.random.split(jax.random.key(seed), 7)
    return {
        "inputs": normal_values(key_of[0], (SEQS, SEQ, D), 1.0, 6.0, ((0, 8), (1, 4))),
        "saved_hidden": normal_values(key_of[1], (SEQS, SEQ, FF), 1.5, 8.0, ((0, 8), (2, 4))),
        "upstream": normal_values(key_of[2], (SEQS, SEQ, D), 1.0, 6.0, ((0, 8), (1, 4))),
        "w_in": normal_values(key_of[3], (D, FF), D ** -0.5, 0.15625, ((1, 4),)),
        "w_out": normal_values(key_of[4], (FF, D), FF ** -0.5, 0.078125, ((0, 4),)),
        "kernel": normal_values(key_of[5], (KW, D), 0.3, 2.0, (), jnp.float32),
    }


def gelu_exact(value):
    return jax.nn.gelu(value, approximate=False)

def one_sequence(carry, items, w_in, w_out, kernel):
    total_in, total_out, total_bias, total_kernel = carry
    inputs, hidden, upstream = items
    length = inputs.shape[0]
    inputs_f = inputs.astype(jnp.float32)
    padded = jnp.pad(inputs_f, ((3, 3), (0, 0)))
    mixed = inputs_f
    for tap in range(KW):
        mixed = mixed + kernel[tap] * padded[tap:tap + length]
    mixed = mixed.astype(jnp.bfloat16)
    hidden_f = hidden.astype(jnp.float32)
    activated = gelu_exact(hidden_f).astype(jnp.bfloat16)
    back_hidden = jnp.dot(upstream, w_out.T, preferred_element_type=jnp.float32)
    grad_hidden = jax.vjp(gelu_exact, hidden_f)[1](back_hidden)[0].astype(jnp.bfloat16)
    total_out = total_out + jnp.dot(activated.T, upstream, preferred_element_type=jnp.float32)
    total_in = total_in + jnp.dot(mixed.T, grad_hidden, preferred_element_type=jnp.float32)
    total_bias = total_bias + lax.optimization_barrier(jnp.sum(grad_hidden.astype(jnp.float32), axis=0))
    block = FF // N_TP
    hidden_blocks = grad_hidden.reshape(length, N_TP, block).astype(jnp.float32)
    weight_blocks = w_in.reshape(D, N_TP, block).astype(jnp.float32)
    parts = jnp.einsum('lnf,dnf->nld', hidden_blocks, weight_blocks).astype(jnp.bfloat16)
    parts = lax.optimization_barrier(parts).astype(jnp.float32)
    grad_mixed = (upstream.astype(jnp.float32) + lax.optimization_barrier(jnp.sum(parts, axis=0))).astype(jnp.bfloat16)
    grad_f = grad_mixed.astype(jnp.float32)
    grad_pad = jnp.pad(grad_f, ((3, 3), (0, 0)))
    grad_inputs = grad_f
    taps = []
    for tap in range(KW):
        grad_inputs = grad_inputs + kernel[tap] * grad_pad[6 - tap:6 - tap + length]
        taps.append(lax.optimization_barrier(jnp.sum(grad_f * padded[tap:tap + length], axis=0)))
    total_kernel = total_kernel + jnp.stack(taps)
    return ((total_in, total_out, total_bias, total_kernel), grad_inputs.astype(jnp.bfloat16))

def reference(inputs, saved_hidden, upstream, w_in, w_out, kernel):
    start = (jnp.zeros((D, FF), jnp.float32), jnp.zeros((FF, D), jnp.float32), jnp.zeros((FF,), jnp.float32), jnp.zeros((KW, D), jnp.float32))
    step = partial(one_sequence, w_in=w_in, w_out=w_out, kernel=kernel)
    totals, grad_inputs = lax.scan(step, start, (inputs, saved_hidden, upstream))
    return (grad_inputs, totals[0], totals[1], totals[2], totals[3])
```

```python
import jax
import jax.numpy as jnp
from jax import lax
from jax.sharding import PartitionSpec as P

KW = 7


def with_halo(cells, sides, width):
    for axis, dim in sides:
        count = lax.axis_size(axis)
        ends = count - 1
        head = lax.slice_in_dim(cells, 0, width, axis=dim)
        tail = lax.slice_in_dim(cells, cells.shape[dim] - width, cells.shape[dim], axis=dim)
        cells = jnp.concatenate(
            [
                lax.ppermute(tail, axis, [(i, (i + 1) % count) for i in range(ends)]),
                cells,
                lax.ppermute(head, axis, [((i + 1) % count, i) for i in range(ends)]),
            ],
            axis=dim,
        )
    return cells


def gelu_exact(value):
    return jax.nn.gelu(value, approximate=False)


def convolve(padded, kernel, length):
    mixed = padded[3 : 3 + length].astype(jnp.float32)
    for tap in range(KW):
        mixed = mixed + kernel[tap] * padded[tap : tap + length].astype(jnp.float32)
    return mixed.astype(jnp.bfloat16)


def line_gather(block, axis):
    count = lax.axis_size(axis)
    index = lax.axis_index(axis)
    length = block.shape[0]
    right = left = block
    rights, lefts = [block], [block]
    for step in range(1, count):
        right = lax.ppermute(right, axis, [(i, i + 1) for i in range(step - 1, count - 1)])
        left = lax.ppermute(left, axis, [(i + 1, i) for i in range(count - step)])
        rights.append(right)
        lefts.append(left)
    whole = jnp.zeros((count * length,) + block.shape[1:], block.dtype)
    whole = lax.dynamic_update_slice_in_dim(whole, block, index * length, 0)
    for step in range(1, count):
        came = rights[step] + lefts[count - step]
        place = lax.rem(index - step + count, count)
        whole = lax.dynamic_update_slice_in_dim(whole, came, place * length, 0)
    return whole


def line_scatter(parts, axis):
    count = lax.axis_size(axis)
    index = lax.axis_index(axis)
    length = parts.shape[0] // count

    def part(place):
        return lax.dynamic_slice_in_dim(
            parts, jnp.clip(place, 0, count - 1) * length, length, 0
        ).astype(jnp.float32)

    right = left = None
    for step in range(count - 1, 0, -1):
        up, down = part(index + step), part(index - step)
        if right is not None:
            up = up + right.astype(jnp.float32)
            down = down + left.astype(jnp.float32)
        right = lax.ppermute(
            up.astype(jnp.bfloat16), axis, [(i, i + 1) for i in range(count - step)]
        )
        left = lax.ppermute(
            down.astype(jnp.bfloat16), axis, [(i, i - 1) for i in range(step, count)]
        )
    total = part(index)
    if right is not None:
        total = total + right.astype(jnp.float32) + left.astype(jnp.float32)
    return total


def pairs(count, mask):
    return [(i, i ^ mask) for i in range(count)]


def masks_of(count):
    return [1 << k for k in range(count.bit_length() - 1)]


def small_sum(value, axes):
    for axis in axes:
        count = lax.axis_size(axis)
        if count & (count - 1):
            value = lax.psum(value, axis)
            continue
        for mask in masks_of(count):
            value = value + lax.ppermute(value, axis, pairs(count, mask))
    return value


def halving_sum(value, axis, flip):
    count = lax.axis_size(axis)
    if count & (count - 1) or value.shape[0] % (16 * count):
        return lax.psum(value.astype(jnp.bfloat16), axis)
    index = lax.axis_index(axis)
    masks = masks_of(count)
    if flip:
        masks = masks[:1] + masks[:0:-1]
    for mask in masks:
        bit = lax.rem(index // mask, 2)
        half = value.shape[0] // 2
        send = lax.dynamic_slice_in_dim(value, (1 - bit) * half, half, 0).astype(jnp.bfloat16)
        keep = lax.dynamic_slice_in_dim(value, bit * half, half, 0).astype(jnp.float32)
        came = lax.ppermute(send, axis, pairs(count, mask))
        value = (keep + came.astype(jnp.float32)).astype(jnp.bfloat16)
    for mask in masks[::-1]:
        bit = lax.rem(index // mask, 2)
        came = lax.ppermute(value, axis, pairs(count, mask))
        value = jnp.where(
            bit == 0, jnp.concatenate([value, came], 0), jnp.concatenate([came, value], 0)
        )
    return value


def weight_sum(value, axis):
    half = value.shape[0] // 2
    return jnp.concatenate(
        [halving_sum(value[:half], axis, False), halving_sum(value[half:], axis, True)], 0
    ).astype(jnp.float32)


def shards(inputs, saved_hidden, upstream, w_in, w_out, kernel):
    tokens = inputs[0]
    hidden = saved_hidden[0]
    grad_out = upstream[0]
    length = tokens.shape[0]
    padded = with_halo(tokens, (("tp", 0),), 3)
    piece = line_gather(grad_out, "tp")
    mixed = convolve(padded, kernel, length)
    mixed_all = line_gather(mixed, "tp")
    hidden_rows = hidden.astype(jnp.float32)
    activated = gelu_exact(hidden_rows).astype(jnp.bfloat16)
    grad_w_out = lax.dot_general(
        activated, piece, (((0,), (0,)), ((), ())), preferred_element_type=jnp.float32
    )
    grad_w_out = weight_sum(grad_w_out, "dp")
    back_rows = lax.dot_general(
        piece, w_out, (((1,), (1,)), ((), ())), preferred_element_type=jnp.float32
    )
    grad_rows = jax.vjp(gelu_exact, hidden_rows)[1](back_rows)[0].astype(jnp.bfloat16)
    grad_bias = small_sum(jnp.sum(grad_rows.astype(jnp.float32), axis=0), ("dp",))
    parts = lax.dot_general(
        grad_rows, w_in, (((1,), (1,)), ((), ())), preferred_element_type=jnp.float32
    ).astype(jnp.bfloat16)
    grad_w_in = lax.dot_general(
        mixed_all, grad_rows, (((0,), (0,)), ((), ())), preferred_element_type=jnp.float32
    )
    grad_w_in = weight_sum(grad_w_in, "dp")
    summed = line_scatter(parts, "tp")
    grad_mixed = (grad_out.astype(jnp.float32) + summed).astype(jnp.bfloat16)
    grad_pad = with_halo(grad_mixed, (("tp", 0),), 3)
    grad_f = grad_mixed.astype(jnp.float32)
    grad_inputs = grad_f
    taps = []
    for tap in range(KW):
        grad_inputs = grad_inputs + kernel[tap] * grad_pad[6 - tap : 6 - tap + length].astype(
            jnp.float32
        )
        taps.append(jnp.sum(grad_f * padded[tap : tap + length].astype(jnp.float32), axis=0))
    grad_kernel = small_sum(jnp.stack(taps), ("tp", "dp"))
    return (grad_inputs.astype(jnp.bfloat16)[None], grad_w_in, grad_w_out, grad_bias, grad_kernel)


def solution(mesh):
    in_specs = (
        P("dp", "tp", None),
        P("dp", None, "tp"),
        P("dp", "tp", None),
        P(None, "tp"),
        P("tp", None),
        P(),
    )
    out_specs = (P("dp", "tp", None), P(None, "tp"), P("tp", None), P("tp"), P())
    return jax.shard_map(shards, mesh=mesh, in_specs=in_specs, out_specs=out_specs, check_vma=False)
```
